1024 devices in a mesh: prow: 16 (over y, core), pcol: 64 (over x, z).
Axes of the slice: x: 8, y: 8, z: 8, core: 2. Of those that a mesh axis runs over, the one named last changes fastest.
Arguments:
- slab: bfloat16 [32768, 24576], P('prow', 'pcol'), may hold values from -6 to 6
- pivots: int32 [512], replicated, may hold values from 0 to 32767, as said below
- l_top: bfloat16 [512, 512], replicated, may hold values from -0.125 to 0.125
- l_panel_t: bfloat16 [512, 32768], P('pcol', 'prow'), may hold values from -0.125 to 0.125
Outputs:
- result: bfloat16 [32768, 24576], P('prow', 'pcol')
The draws below stay inside these ranges and needn't reach their ends.
Inputs may be any that keep to these rules, and one draw needn't show every extreme that they name: `pivots`: distinct rows; how many fall on each index of prow is uneven and changes with the draw.
All inputs are finite; a program needn't handle non-finite values.
Results may differ from the reference program's by a relative error of at most 0.0029.
Values may be sent and summed in bfloat16 or wider, within the bound.
No kernel may reach another device: no remote copies, remote signals or barrier semaphores. Data moves between devices by JAX's collectives and lax.ppermute only.
A program may use at most 64 MiB of HBM per device.

```python
import jax
import jax.numpy as jnp
from jax import lax

NB = 512
ROW_DEV = 2048
ROWS = 32768
COLS = 24576
N_PROW = 16


def draw_pivots(key, part):
    first_key, second_key, third_key = jax.random.split(key, 3)
    weights = jax.random.randint(first_key, (N_PROW,), 1, 9)
    cumulative = jnp.cumsum(weights)
    picks = jax.random.randint(second_key, (NB,), 0, cumulative[-1])
    owner = jnp.sum((picks[:, None] >= cumulative[None, :]).astype(jnp.int32), axis=1)
    onehot = (owner[:, None] == jnp.arange(N_PROW, dtype=jnp.int32)[None, :]).astype(jnp.int32)
    ranks = jnp.sum((jnp.cumsum(onehot, axis=0) - onehot) * onehot, axis=1)
    owner_keys = jax.random.split(third_key, N_PROW)
    orders = jax.vmap(lambda k: jax.random.permutation(k, ROW_DEV))(owner_keys)
    local = orders[owner, ranks]
    return (owner * ROW_DEV + local).astype(jnp.int32)


def shard_levels(rng, extent, pieces, low, high):
    def one(position, shards_of):
        heights = jax.random.uniform(jax.random.fold_in(jax.random.fold_in(rng, 6), position), (shards_of,), jnp.float32, low / len(pieces), high / len(pieces))
        return jnp.repeat(jnp.exp(heights), extent[position] // shards_of).reshape((-1,) + (1,) * (len(extent) - position - 1))

    level = one(*pieces[0])
    for cut in pieces[1:]:
        level = level * one(*cut)
    return level


def centred(stream_key, dims, deviation, reach, shards=(), kind=jnp.bfloat16):
    entries = jax.random.normal(stream_key, dims, jnp.float32) * deviation
    if len(shards) > 0:
        entries = shard_levels(stream_key, dims, shards, -0.22, 0.18) * entries
    return jnp.clip(entries, min=-reach, max=reach).astype(kind)


def setup_inputs(seed: int = 0) -> dict:
    streams_of = jax.random.split(jax.random.key(seed), 5)
    return {
        "slab": centred(streams_of[0], (ROWS, COLS), 1.0, 6.0, ((0, 16), (1, 64))),
        "pivots": draw_pivots(jax.random.fold_in(streams_of[4], 71), 0),
        "l_top": centred(streams_of[2], (NB, NB), (4 * NB) ** -0.5, 0.125),
        "l_panel_t": centred(streams_of[3], (NB, ROWS), (4 * NB) ** -0.5, 0.125, ((0, 64), (1, 16))),
    }


def bookkeeping(pivots):
    index = jnp.arange(NB, dtype=jnp.int32)
    chosen = jnp.any(pivots[:, None] == index[None, :], axis=0)
    free = jnp.logical_not(chosen)
    free_rank = jnp.cumsum(free.astype(jnp.int32)) - 1
    far = pivots >= NB
    far_rank = jnp.cumsum(far.astype(jnp.int32)) - 1
    match = free[None, :] & (free_rank[None, :] == far_rank[:, None])
    source = jnp.sum(jnp.where(match, index[None, :], 0), axis=1).astype(jnp.int32)
    return (far, source)

def reference(slab, pivots, l_top, l_panel_t):
    total_rows = slab.shape[0]
    far, source = bookkeeping(pivots)
    target = jnp.where(far, pivots, total_rows).astype(jnp.int32)
    pivoted = slab.at[target].set(slab[source], mode='drop')
    top = slab[pivots]
    lower = jnp.tril(l_top.astype(jnp.float32), -1) + jnp.eye(NB, dtype=jnp.float32)
    upper = lax.linalg.triangular_solve(lower, top.astype(jnp.float32), left_side=True, lower=True, unit_diagonal=True)
    u_block = upper.astype(jnp.bfloat16)
    u_wide = u_block.astype(jnp.float32)
    blocks = pivoted.reshape(N_PROW, ROW_DEV, -1)
    panels = jnp.transpose(l_panel_t.reshape(NB, N_PROW, ROW_DEV), (1, 0, 2))

    def one_block(pair):
        rows_here, panel_here = pair
        product = jnp.dot(panel_here.astype(jnp.float32).T.astype(jnp.float32), u_wide.astype(jnp.float32), preferred_element_type=jnp.float32)
        return (rows_here.astype(jnp.float32) - product).astype(jnp.bfloat16)
    updated = lax.map(one_block, (blocks, panels)).reshape(total_rows, -1)
    return updated.at[:NB].set(u_block)
```

```python
import jax
import jax.numpy as jnp
from jax import lax
from jax.experimental import pallas as pl
from jax.experimental.pallas import tpu as pltpu
from jax.sharding import PartitionSpec as P

BF, F32 = jnp.bfloat16, jnp.float32
HI = lax.Precision.HIGHEST


def bookkeeping(pivots, block):
    index = jnp.arange(block, dtype=jnp.int32)
    chosen = jnp.any(pivots[:, None] == index[None, :], axis=0)
    free = jnp.logical_not(chosen)
    below = index[:, None] < index[None, :]
    free_rank = jnp.sum((free[:, None] & below).astype(jnp.int32), axis=0)
    far = pivots >= block
    far_rank = jnp.sum((far[:, None] & below).astype(jnp.int32), axis=0)
    match = free[None, :] & (free_rank[None, :] == far_rank[:, None])
    source = jnp.sum(jnp.where(match, index[None, :], 0), axis=1)
    return far, source


def mm(a, b):
    return jnp.dot(a, b, precision=HI, preferred_element_type=F32)


def inverse_kernel(l_ref, a_ref, b_ref, c_ref, x_ref):
    n, t = l_ref.shape[0], 128
    row = lax.broadcasted_iota(jnp.int32, (t, t), 0)
    col = lax.broadcasted_iota(jnp.int32, (t, t), 1)
    eye = (row == col).astype(F32)
    x_ref[...] = jnp.zeros_like(x_ref)
    blocks = range(n // t)
    low = [
        jnp.where(row > col, l_ref[b * t : (b + 1) * t, b * t : (b + 1) * t].astype(F32), 0.0)
        for b in blocks
    ]
    step = 16
    near = [jnp.where(row // step == col // step, v, 0.0) for v in low]
    inv = [eye - v for v in near]
    power = near
    for _ in range(3):
        power = [mm(v, v) for v in power]
        inv = [x + mm(x, v) for x, v in zip(inv, power)]
    while step < t:
        off = [
            jnp.where((row // (2 * step) == col // (2 * step)) & (row // step != col // step), v, 0.0)
            for v in low
        ]
        half = [mm(x, v) for x, v in zip(inv, off)]
        inv = [x - mm(h, x) for x, h in zip(inv, half)]
        step *= 2
    for b in blocks:
        x_ref[b * t : (b + 1) * t, b * t : (b + 1) * t] = inv[b]
    size = t
    while size < n:
        for s in range(0, n, 2 * size):
            top, bot = slice(s, s + size), slice(s + size, s + 2 * size)
            x_ref[bot, top] = -mm(x_ref[bot, bot], mm(l_ref[bot, top].astype(F32), x_ref[top, top]))
        size *= 2
    x = x_ref[...]
    a = x.astype(BF)
    a_ref[...] = a
    x = x - a.astype(F32)
    b = x.astype(BF)
    b_ref[...] = b
    c_ref[...] = (x - b.astype(F32)).astype(BF)


def inverse(l_top):
    n = l_top.shape[0]
    shape = jax.ShapeDtypeStruct((n, n), BF)
    return pl.pallas_call(
        inverse_kernel,
        out_shape=[shape] * 3,
        scratch_shapes=[pltpu.VMEM((n, n), F32)],
        cost_estimate=pl.CostEstimate(flops=2 * 10**9, bytes_accessed=4 * n * n * 2, transcendentals=0),
    )(l_top)


def solve_kernel(row_ref, a_ref, b_ref, c_ref, top_ref, u_ref, v_ref):
    top = top_ref[...]
    u = jnp.dot(c_ref[...], top, preferred_element_type=F32)
    u += jnp.dot(b_ref[...], top, preferred_element_type=F32)
    u += jnp.dot(a_ref[...], top, preferred_element_type=F32)
    u_ref[...] = u.astype(BF)
    v_ref[...] = u.astype(BF)

    @pl.when(row_ref[0] % 2 == 1)
    def _():
        v = [u[(8 * x + z) * 8 : (8 * x + z + 1) * 8] for z in range(8) for x in range(8)]
        v_ref[...] = jnp.concatenate(v, axis=0).astype(BF)


def solve(row, parts, top):
    shape = jax.ShapeDtypeStruct(top.shape, BF)
    return pl.pallas_call(
        solve_kernel,
        in_specs=[pl.BlockSpec(memory_space=pltpu.SMEM)] + [pl.BlockSpec(memory_space=pltpu.VMEM)] * 4,
        out_shape=[shape] * 2,
        cost_estimate=pl.CostEstimate(flops=10**9, bytes_accessed=10**7, transcendentals=0),
    )(row, *parts, top)


def update_kernel(row_ref, l_ref, u_ref, v_ref, target_ref, home_ref, slab_ref, out_ref):
    j = pl.program_id(0)
    rows = slab_ref.shape[0]
    n = u_ref.shape[0]
    index = j * rows + lax.broadcasted_iota(jnp.int32, (rows, n), 0)
    hit = index == target_ref[...]
    lost = jnp.any(hit, axis=1, keepdims=True)
    put = jnp.dot(hit.astype(BF), home_ref[...], preferred_element_type=F32)
    base = jnp.where(lost, put, slab_ref[...].astype(F32))
    product = lax.dot_general(l_ref[...], v_ref[...], (((0,), (0,)), ((), ())), preferred_element_type=F32)
    out_ref[...] = (base - product).astype(BF)

    @pl.when((row_ref[0] == 0) & (j * rows < n))
    def _():
        out_ref[...] = u_ref[pl.ds(pl.multiple_of(jnp.minimum(j * rows, n - rows), rows), rows), :]


def update(row, panel, u, v, target, home, slab, rows):
    n, height = panel.shape
    w = slab.shape[1]
    whole = lambda a: pl.BlockSpec(a.shape, lambda j: (0,) * a.ndim)
    return pl.pallas_call(
        update_kernel,
        grid=(height // rows,),
        in_specs=[
            pl.BlockSpec(memory_space=pltpu.SMEM),
            pl.BlockSpec((n, rows), lambda j: (0, j)),
            whole(u), whole(v), whole(target), whole(home),
            pl.BlockSpec((rows, w), lambda j: (j, 0)),
        ],
        out_specs=pl.BlockSpec((rows, w), lambda j: (j, 0)),
        out_shape=jax.ShapeDtypeStruct(slab.shape, BF),
        cost_estimate=pl.CostEstimate(
            flops=4 * height * n * w, bytes_accessed=2 * n * height + 4 * height * w, transcendentals=0
        ),
    )(row, panel, u, v, target, home, slab)


def lines(first):
    groups = []
    for row in range(16):
        for i in range(8):
            line = [i * 8 + j if row % 2 == first else j * 8 + i for j in range(8)]
            groups.append([row * 64 + c for c in line])
    return groups


def exchange(block, groups):
    copies = jnp.broadcast_to(block[None], (8,) + block.shape)
    return lax.all_to_all(copies, ("prow", "pcol"), 0, 0, axis_index_groups=groups)


def per_device(slab, pivots, l_top, l_panel_t):
    local_rows, w = slab.shape
    n = pivots.shape[0]
    k = l_panel_t.shape[0]
    row = lax.axis_index("prow")
    r = row.reshape(1).astype(jnp.int32)
    near = exchange(l_panel_t, lines(0)).reshape(8 * k, local_rows)
    parts = inverse(l_top)

    far, source = bookkeeping(pivots, n)
    owner = pivots // local_rows
    local = pivots - row * local_rows
    mine = owner == row
    pick = jnp.where(mine, local, jnp.where(row == 0, source, 0))
    picked = slab[pick]
    p = 16
    chunk = n // p
    picked, near = lax.optimization_barrier((picked, near))
    got = lax.all_to_all(picked.reshape(p, chunk, w), "prow", 0, 0)
    here = lax.dynamic_slice(owner, (row * chunk,), (chunk,))
    chosen = here[None, :] == jnp.arange(p, dtype=jnp.int32)[:, None]
    got, near = lax.optimization_barrier((got, near))
    panel = exchange(near, lines(1)).reshape(n, local_rows)
    top_part = jnp.sum(jnp.where(chosen[:, :, None], got.astype(F32), 0.0), axis=0).astype(BF)
    both = lax.all_gather(jnp.stack([top_part, got[0]]), "prow", axis=0)
    top = both[:, 0].reshape(n, w)
    home = jnp.where(row == 0, slab[source], both[:, 1].reshape(n, w))
    u, v = solve(r, parts, top)
    target = jnp.where(far & mine, local, local_rows)[None, :]
    return update(r, panel, u, v, target, home, slab, 256)


def solution(mesh):
    return jax.shard_map(
        per_device,
        mesh=mesh,
        in_specs=(P("prow", "pcol"), P(), P(), P("pcol", "prow")),
        out_specs=P("prow", "pcol"),
        check_vma=False,
    )
```

```python
import jax
import jax.numpy as jnp
from jax import lax
from jax.experimental import pallas as pl
from jax.experimental.pallas import tpu as pltpu
from jax.sharding import PartitionSpec as P


BF, F32 = jnp.bfloat16, jnp.float32
HI = lax.Precision.HIGHEST


CAP = 80
ROOM = pltpu.CompilerParams(vmem_limit_bytes=20 * 2**20)


def column(row):
    n = row.shape[1]
    eye = lax.broadcasted_iota(jnp.int32, (n, n), 0) == lax.broadcasted_iota(jnp.int32, (n, n), 1)
    return jnp.sum(jnp.where(eye, row, 0.0), axis=1, keepdims=True)


def pick_kernel(where_ref, pivot_ref, slab_ref, pick_ref, place_ref, dest_ref, most_ref):
    n, rows = pivot_ref.shape[1], slab_ref.shape[0]
    me, base = where_ref[0], where_ref[1].astype(F32)
    p_int = pivot_ref[...]
    p_row = p_int.astype(F32)
    p_col = column(p_row)
    o_row = (p_int // rows).astype(F32)
    o_col = column(o_row)
    sub = lax.broadcasted_iota(jnp.int32, (n, n), 0)
    lane = lax.broadcasted_iota(jnp.int32, (n, n), 1)
    same = o_col == o_row
    rank_row = jnp.sum(jnp.where(same & (sub < lane), 1.0, 0.0), axis=0, keepdims=True)
    rank_col = jnp.sum(jnp.where(same & (lane < sub), 1.0, 0.0), axis=1, keepdims=True)
    most_ref[0] = jnp.max(rank_row).astype(jnp.int32) + 1
    slot = rank_col - base
    place_ref[...] = jnp.where((slot >= 0) & (slot < CAP), o_col * CAP + slot, -1.0).astype(jnp.int32)

    index = lax.broadcasted_iota(jnp.int32, (CAP, n), 0).astype(F32) + base
    chosen = (o_row == me.astype(F32)) & (rank_row == index)
    local = jnp.sum(jnp.where(chosen, p_row - (me * rows).astype(F32), 0.0), axis=1, keepdims=True)
    hot = lax.broadcasted_iota(jnp.int32, (CAP, rows), 1) == local.astype(jnp.int32)
    pick_ref[...] = jnp.dot(hot.astype(BF), slab_ref[...], preferred_element_type=F32).astype(BF)

    taken = jnp.where(p_col == lane.astype(F32), 1.0, 0.0)
    free_row = 1.0 - jnp.max(taken, axis=0, keepdims=True)
    free_col = column(free_row)
    far_row = jnp.where(p_row >= n, 1.0, 0.0)
    far_col = jnp.where(p_col >= n, 1.0, 0.0)
    free_rank = jnp.sum(jnp.where(sub < lane, free_col, 0.0), axis=0, keepdims=True)
    far_rank = jnp.sum(jnp.where(lane < sub, far_row, 0.0), axis=1, keepdims=True)
    match = (far_rank == free_rank) & (far_col > 0) & (free_row > 0)
    dest_ref[...] = (jnp.sum(jnp.where(match, p_col + 1.0, 0.0), axis=0, keepdims=True) - 1.0).astype(jnp.int32)


def pick(where, pivots, slab):
    n, w = pivots.shape[0], slab.shape[1]
    vmem = pl.BlockSpec(memory_space=pltpu.VMEM)
    return pl.pallas_call(
        pick_kernel,
        in_specs=[pl.BlockSpec(memory_space=pltpu.SMEM), vmem, vmem],
        out_shape=[
            jax.ShapeDtypeStruct((CAP, w), BF),
            jax.ShapeDtypeStruct((n, 1), jnp.int32),
            jax.ShapeDtypeStruct((1, n), jnp.int32),
            jax.ShapeDtypeStruct((1,), jnp.int32),
        ],
        out_specs=[vmem, vmem, vmem, pl.BlockSpec(memory_space=pltpu.SMEM)],
        compiler_params=ROOM,
        cost_estimate=pl.CostEstimate(flops=2 * 10**9, bytes_accessed=2 * slab.size, transcendentals=0),
    )(where, pivots[None], slab)


def mm(a, b):
    return jnp.dot(a, b, precision=HI, preferred_element_type=F32)


def inverse_kernel(l_ref, a_ref, b_ref, x_ref):
    n, t = l_ref.shape[0], 128
    row = lax.broadcasted_iota(jnp.int32, (t, t), 0)
    col = lax.broadcasted_iota(jnp.int32, (t, t), 1)
    eye = (row == col).astype(F32)
    x_ref[...] = jnp.zeros_like(x_ref)
    blocks = range(n // t)
    low = [
        jnp.where(row > col, l_ref[b * t : (b + 1) * t, b * t : (b + 1) * t].astype(F32), 0.0)
        for b in blocks
    ]
    step = 16
    near = [jnp.where(row // step == col // step, v, 0.0) for v in low]
    inv = [eye - v for v in near]
    power = near
    for _ in range(3):
        power = [mm(v, v) for v in power]
        inv = [x + mm(x, v) for x, v in zip(inv, power)]
    while step < t:
        off = [
            jnp.where((row // (2 * step) == col // (2 * step)) & (row // step != col // step), v, 0.0)
            for v in low
        ]
        half = [mm(x, v) for x, v in zip(inv, off)]
        inv = [x - mm(h, x) for x, h in zip(inv, half)]
        step *= 2
    for b in blocks:
        x_ref[b * t : (b + 1) * t, b * t : (b + 1) * t] = inv[b]
    size = t
    while size < n:
        for s in range(0, n, 2 * size):
            top, bot = slice(s, s + size), slice(s + size, s + 2 * size)
            x_ref[bot, top] = -mm(x_ref[bot, bot], mm(l_ref[bot, top].astype(F32), x_ref[top, top]))
        size *= 2
    x = x_ref[...]
    a = x.astype(BF)
    a_ref[...] = a
    b_ref[...] = (x - a.astype(F32)).astype(BF)


def inverse(l_top):
    n = l_top.shape[0]
    shape = jax.ShapeDtypeStruct((n, n), BF)
    return pl.pallas_call(
        inverse_kernel,
        out_shape=[shape] * 2,
        scratch_shapes=[pltpu.VMEM((n, n), F32)],
        compiler_params=ROOM,
        cost_estimate=pl.CostEstimate(flops=2 * 10**9, bytes_accessed=4 * n * n * 2, transcendentals=0),
    )(l_top)


def placed(place_ref, got_ref):
    hot = lax.broadcasted_iota(jnp.int32, (place_ref.shape[0], got_ref.shape[0]), 1) == place_ref[...]
    return jnp.dot(hot.astype(BF), got_ref[...], preferred_element_type=F32)


def finish(row_ref, a_ref, b_ref, top, u_ref, v_ref):
    u = jnp.dot(b_ref[...], top, preferred_element_type=F32)
    u += jnp.dot(a_ref[...], top, preferred_element_type=F32)
    u_ref[...] = u.astype(BF)
    v_ref[...] = (-u).astype(BF)

    @pl.when(row_ref[0] % 2 == 1)
    def _():
        v = [u[(8 * x + z) * 8 : (8 * x + z + 1) * 8] for z in range(8) for x in range(8)]
        v_ref[...] = (-jnp.concatenate(v, axis=0)).astype(BF)


def place_solve_kernel(row_ref, a_ref, b_ref, place_ref, got_ref, u_ref, v_ref):
    finish(row_ref, a_ref, b_ref, placed(place_ref, got_ref).astype(BF), u_ref, v_ref)


def solve_kernel(row_ref, a_ref, b_ref, top_ref, u_ref, v_ref):
    finish(row_ref, a_ref, b_ref, top_ref[...], u_ref, v_ref)


def add_kernel(top_ref, place_ref, got_ref, out_ref):
    out_ref[...] = (top_ref[...].astype(F32) + placed(place_ref, got_ref)).astype(BF)


def solve(kernel, row, parts, *rest):
    n, w = parts[0].shape[0], rest[-1].shape[1]
    shape = jax.ShapeDtypeStruct((n, w), BF)
    vmem = pl.BlockSpec(memory_space=pltpu.VMEM)
    return tuple(pl.pallas_call(
        kernel,
        in_specs=[pl.BlockSpec(memory_space=pltpu.SMEM)] + [vmem] * (2 + len(rest)),
        out_shape=[shape] * 2,
        compiler_params=ROOM,
        cost_estimate=pl.CostEstimate(flops=10**9, bytes_accessed=10**7, transcendentals=0),
    )(row, *parts, *rest))


def update_kernel(row_ref, l_ref, u_ref, v_ref, dest_ref, own_ref, sent_ref, slab_ref, out_ref, right_ref):
    j = pl.program_id(0)
    rows, w = slab_ref.shape
    n = u_ref.shape[0]

    @pl.when(j == 0)
    def _():
        right_ref[:n, :w] = v_ref[...]
        right_ref[:n, w:] = jnp.zeros_like(right_ref[:n, w:])
        right_ref[n:, w:] = jnp.ones_like(right_ref[n:, w:])

        @pl.when(row_ref[0] % 2 == 0)
        def _():
            right_ref[n:, :w] = own_ref[...]

        @pl.when(row_ref[0] % 2 == 1)
        def _():
            right_ref[n:, :w] = sent_ref[...]

    first = (row_ref[0] * pl.num_programs(0) + j) * rows
    hit = first + lax.broadcasted_iota(jnp.int32, (rows, n), 0) == dest_ref[...]
    left = jnp.concatenate([l_ref[...].T, hit.astype(BF)], axis=1)
    acc = jnp.dot(left, right_ref[...], preferred_element_type=F32)
    lost = jnp.concatenate([acc[:, w:]] * (w // 128), axis=1)
    out_ref[...] = (jnp.where(lost > 0, 0.0, slab_ref[...].astype(F32)) + acc[:, :w]).astype(BF)

    @pl.when((row_ref[0] == 0) & (j * rows < n))
    def _():
        out_ref[...] = u_ref[pl.ds(pl.multiple_of(jnp.minimum(j * rows, n - rows), rows), rows), :]


def update(row, panel, u, v, dest, own, sent, slab, rows):
    n, height = panel.shape
    w = slab.shape[1]
    whole = lambda a: pl.BlockSpec(a.shape, lambda j: (0,) * a.ndim)
    return pl.pallas_call(
        update_kernel,
        grid=(height // rows,),
        in_specs=[
            pl.BlockSpec(memory_space=pltpu.SMEM),
            pl.BlockSpec((n, rows), lambda j: (0, j)),
            *map(whole, (u, v, dest, own, sent)),
            pl.BlockSpec((rows, w), lambda j: (j, 0)),
        ],
        out_specs=pl.BlockSpec((rows, w), lambda j: (j, 0)),
        out_shape=jax.ShapeDtypeStruct(slab.shape, BF),
        scratch_shapes=[pltpu.VMEM((2 * n, w + 128), BF)],
        compiler_params=ROOM,
        cost_estimate=pl.CostEstimate(
            flops=4 * height * n * w, bytes_accessed=2 * n * height + 4 * height * w, transcendentals=0
        ),
    )(row, panel, u, v, dest, own, sent, slab)


def lines(first):
    groups = []
    for row in range(16):
        for i in range(8):
            line = [i * 8 + j if row % 2 == first else j * 8 + i for j in range(8)]
            groups.append([row * 64 + c for c in line])
    return groups


def exchange(block, groups):
    copies = jnp.broadcast_to(block[None], (8,) + block.shape)
    return lax.all_to_all(copies, ("prow", "pcol"), 0, 0, axis_index_groups=groups)


def hand_on(home, size):
    return lax.ppermute(home, "prow", [(i, i + size // 2) for i in range(0, 16, size)])


def step_of_panel(slab, pivots, l_top, l_panel_t):
    local_rows, w = slab.shape
    n = pivots.shape[0]
    k = l_panel_t.shape[0]
    row = lax.axis_index("prow").astype(jnp.int32)
    r = row.reshape(1)

    def picks(base):
        return pick(jnp.stack([row, base]), pivots, slab)

    near = exchange(l_panel_t, lines(0)).reshape(8 * k, local_rows)
    home = slab[:n]
    got = hand_on(home, 16)
    parts = inverse(l_top)
    got, parts = lax.optimization_barrier((got, parts))
    home = jnp.where(row == 0, home, got)
    got = hand_on(home, 8)
    picked, place, dest, most = picks(jnp.int32(0))
    near, got, picked = lax.optimization_barrier((near, got, picked))
    home = jnp.where(row % 8 == 0, home, got)
    got = hand_on(home, 4)
    panel = exchange(near, lines(1)).reshape(n, local_rows)
    got, picked = lax.optimization_barrier((got, picked))
    home = jnp.where(row % 4 == 0, home, got)
    sent = hand_on(home, 2)
    got = lax.all_gather(picked, "prow", axis=0, tiled=True)

    def direct():
        return solve(place_solve_kernel, r, parts, place, got)

    def in_rounds():
        def step(state):
            base, top = state
            picked, place, _, _ = picks(base)
            got = lax.all_gather(picked, "prow", axis=0, tiled=True)
            top = pl.pallas_call(add_kernel, out_shape=jax.ShapeDtypeStruct((n, w), BF))(top, place, got)
            return base + CAP, top

        _, top = lax.while_loop(lambda s: s[0] < most[0], step, (jnp.int32(0), jnp.zeros((n, w), BF)))
        return solve(solve_kernel, r, parts, top)

    u, v = lax.cond(most[0] <= CAP, direct, in_rounds)
    return update(r, panel, u, v, dest, home, sent, slab, 256)


def solution(mesh):
    return jax.shard_map(
        step_of_panel,
        mesh=mesh,
        in_specs=(P("prow", "pcol"), P(), P(), P("pcol", "prow")),
        out_specs=P("prow", "pcol"),
        check_vma=False,
    )
```

```python
import jax
import jax.numpy as jnp
from jax import lax
from jax.experimental import pallas as pl
from jax.experimental.pallas import tpu as pltpu
from jax.sharding import PartitionSpec as P


BF, F32 = jnp.bfloat16, jnp.float32
HI = lax.Precision.HIGHEST


CAP = 80
ROOM = pltpu.CompilerParams(vmem_limit_bytes=20 * 2**20)


def column(row):
    n = row.shape[1]
    eye = lax.broadcasted_iota(jnp.int32, (n, n), 0) == lax.broadcasted_iota(jnp.int32, (n, n), 1)
    return jnp.sum(jnp.where(eye, row, 0.0), axis=1, keepdims=True)


def pick_kernel(where_ref, pivot_ref, slab_ref, pick_ref, place_ref, dest_ref, most_ref):
    n, rows = pivot_ref.shape[1], slab_ref.shape[0]
    me, base = where_ref[0], where_ref[1].astype(F32)
    p_int = pivot_ref[...]
    p_row = p_int.astype(F32)
    p_col = column(p_row)
    o_row = (p_int // rows).astype(F32)
    o_col = column(o_row)
    sub = lax.broadcasted_iota(jnp.int32, (n, n), 0)
    lane = lax.broadcasted_iota(jnp.int32, (n, n), 1)
    same = o_col == o_row
    rank_row = jnp.sum(jnp.where(same & (sub < lane), 1.0, 0.0), axis=0, keepdims=True)
    rank_col = jnp.sum(jnp.where(same & (lane < sub), 1.0, 0.0), axis=1, keepdims=True)
    most_ref[0] = jnp.max(rank_row).astype(jnp.int32) + 1
    slot = rank_col - base
    place_ref[...] = jnp.where((slot >= 0) & (slot < CAP), o_col * CAP + slot, -1.0).astype(jnp.int32)

    index = lax.broadcasted_iota(jnp.int32, (CAP, n), 0).astype(F32) + base
    chosen = (o_row == me.astype(F32)) & (rank_row == index)
    local = jnp.sum(jnp.where(chosen, p_row - (me * rows).astype(F32), 0.0), axis=1, keepdims=True)
    hot = lax.broadcasted_iota(jnp.int32, (CAP, rows), 1) == local.astype(jnp.int32)
    pick_ref[...] = jnp.dot(hot.astype(BF), slab_ref[...], preferred_element_type=F32).astype(BF)

    taken = jnp.where(p_col == lane.astype(F32), 1.0, 0.0)
    free_row = 1.0 - jnp.max(taken, axis=0, keepdims=True)
    free_col = column(free_row)
    far_row = jnp.where(p_row >= n, 1.0, 0.0)
    far_col = jnp.where(p_col >= n, 1.0, 0.0)
    free_rank = jnp.sum(jnp.where(sub < lane, free_col, 0.0), axis=0, keepdims=True)
    far_rank = jnp.sum(jnp.where(lane < sub, far_row, 0.0), axis=1, keepdims=True)
    match = (far_rank == free_rank) & (far_col > 0) & (free_row > 0)
    dest_ref[...] = (jnp.sum(jnp.where(match, p_col + 1.0, 0.0), axis=0, keepdims=True) - 1.0).astype(jnp.int32)


def pick(where, pivots, slab):
    n, w = pivots.shape[0], slab.shape[1]
    vmem = pl.BlockSpec(memory_space=pltpu.VMEM)
    return pl.pallas_call(
        pick_kernel,
        in_specs=[pl.BlockSpec(memory_space=pltpu.SMEM), vmem, vmem],
        out_shape=[
            jax.ShapeDtypeStruct((CAP, w), BF),
            jax.ShapeDtypeStruct((n, 1), jnp.int32),
            jax.ShapeDtypeStruct((1, n), jnp.int32),
            jax.ShapeDtypeStruct((1,), jnp.int32),
        ],
        out_specs=[vmem, vmem, vmem, pl.BlockSpec(memory_space=pltpu.SMEM)],
        compiler_params=ROOM,
        cost_estimate=pl.CostEstimate(flops=2 * 10**9, bytes_accessed=2 * slab.size, transcendentals=0),
    )(where, pivots[None], slab)


def mm(a, b):
    return jnp.dot(a, b, precision=HI, preferred_element_type=F32)


def inverse_kernel(l_ref, a_ref, b_ref, x_ref):
    n, t = l_ref.shape[0], 128
    row = lax.broadcasted_iota(jnp.int32, (t, t), 0)
    col = lax.broadcasted_iota(jnp.int32, (t, t), 1)
    eye = (row == col).astype(F32)
    x_ref[...] = jnp.zeros_like(x_ref)
    blocks = range(n // t)
    low = [
        jnp.where(row > col, l_ref[b * t : (b + 1) * t, b * t : (b + 1) * t].astype(F32), 0.0)
        for b in blocks
    ]
    step = 16
    near = [jnp.where(row // step == col // step, v, 0.0) for v in low]
    inv = [eye - v for v in near]
    power = near
    for _ in range(3):
        power = [mm(v, v) for v in power]
        inv = [x + mm(x, v) for x, v in zip(inv, power)]
    while step < t:
        off = [
            jnp.where((row // (2 * step) == col // (2 * step)) & (row // step != col // step), v, 0.0)
            for v in low
        ]
        half = [mm(x, v) for x, v in zip(inv, off)]
        inv = [x - mm(h, x) for x, h in zip(inv, half)]
        step *= 2
    for b in blocks:
        x_ref[b * t : (b + 1) * t, b * t : (b + 1) * t] = inv[b]
    size = t
    while size < n:
        for s in range(0, n, 2 * size):
            top, bot = slice(s, s + size), slice(s + size, s + 2 * size)
            x_ref[bot, top] = -mm(x_ref[bot, bot], mm(l_ref[bot, top].astype(F32), x_ref[top, top]))
        size *= 2
    x = x_ref[...]
    a = x.astype(BF)
    a_ref[...] = a
    b_ref[...] = (x - a.astype(F32)).astype(BF)


def inverse(l_top):
    n = l_top.shape[0]
    shape = jax.ShapeDtypeStruct((n, n), BF)
    return pl.pallas_call(
        inverse_kernel,
        out_shape=[shape] * 2,
        scratch_shapes=[pltpu.VMEM((n, n), F32)],
        compiler_params=ROOM,
        cost_estimate=pl.CostEstimate(flops=2 * 10**9, bytes_accessed=4 * n * n * 2, transcendentals=0),
    )(l_top)


def placed(place_ref, got_ref):
    hot = lax.broadcasted_iota(jnp.int32, (place_ref.shape[0], got_ref.shape[0]), 1) == place_ref[...]
    return jnp.dot(hot.astype(BF), got_ref[...], preferred_element_type=F32)


def finish(row_ref, a_ref, b_ref, top, u_ref, v_ref):
    u = jnp.dot(b_ref[...], top, preferred_element_type=F32)
    u += jnp.dot(a_ref[...], top, preferred_element_type=F32)
    u_ref[...] = u.astype(BF)
    v_ref[...] = (-u).astype(BF)

    @pl.when(row_ref[0] % 2 == 1)
    def _():
        v = [u[(8 * x + z) * 8 : (8 * x + z + 1) * 8] for z in range(8) for x in range(8)]
        v_ref[...] = (-jnp.concatenate(v, axis=0)).astype(BF)


def place_solve_kernel(row_ref, a_ref, b_ref, place_ref, got_ref, u_ref, v_ref):
    finish(row_ref, a_ref, b_ref, placed(place_ref, got_ref).astype(BF), u_ref, v_ref)


def solve_kernel(row_ref, a_ref, b_ref, top_ref, u_ref, v_ref):
    finish(row_ref, a_ref, b_ref, top_ref[...], u_ref, v_ref)


def add_kernel(top_ref, place_ref, got_ref, out_ref):
    out_ref[...] = (top_ref[...].astype(F32) + placed(place_ref, got_ref)).astype(BF)


def solve(kernel, row, parts, *rest):
    n, w = parts[0].shape[0], rest[-1].shape[1]
    shape = jax.ShapeDtypeStruct((n, w), BF)
    vmem = pl.BlockSpec(memory_space=pltpu.VMEM)
    return tuple(pl.pallas_call(
        kernel,
        in_specs=[pl.BlockSpec(memory_space=pltpu.SMEM)] + [vmem] * (2 + len(rest)),
        out_shape=[shape] * 2,
        compiler_params=ROOM,
        cost_estimate=pl.CostEstimate(flops=10**9, bytes_accessed=10**7, transcendentals=0),
    )(row, *parts, *rest))


def swap_kernel(row_ref, dest_ref, own_ref, sent_ref, slab_ref, out_ref, right_ref):
    j = pl.program_id(0)
    rows, w = slab_ref.shape
    n = own_ref.shape[0]

    @pl.when(j == 0)
    def _():
        right_ref[:, w:] = jnp.ones_like(right_ref[:, w:])

        @pl.when(row_ref[0] % 2 == 0)
        def _():
            right_ref[:, :w] = own_ref[...]

        @pl.when(row_ref[0] % 2 == 1)
        def _():
            right_ref[:, :w] = sent_ref[...]

    first = (row_ref[0] * pl.num_programs(0) + j) * rows
    hit = first + lax.broadcasted_iota(jnp.int32, (rows, n), 0) == dest_ref[...]
    acc = jnp.dot(hit.astype(BF), right_ref[...], preferred_element_type=F32)
    lost = jnp.concatenate([acc[:, w:]] * (w // 128), axis=1)
    out_ref[...] = jnp.where(lost > 0, acc[:, :w].astype(BF), slab_ref[...])


def update_kernel(row_ref, l_ref, u_ref, v_ref, slab_ref, out_ref):
    j = pl.program_id(0)
    rows, n = slab_ref.shape[0], u_ref.shape[0]
    acc = jnp.dot(l_ref[...].T, v_ref[...], preferred_element_type=F32)
    out_ref[...] = (slab_ref[...].astype(F32) + acc).astype(BF)

    @pl.when((row_ref[0] == 0) & (j * rows < n))
    def _():
        out_ref[...] = u_ref[pl.ds(pl.multiple_of(jnp.minimum(j * rows, n - rows), rows), rows), :]


def by_rows(kernel, rows, out, args, flops, scratch=(), alias=()):
    specs = [pl.BlockSpec(memory_space=pltpu.SMEM)]
    for a in args[1:]:
        if not isinstance(a, tuple):
            specs.append(pl.BlockSpec(a.shape, lambda j: (0, 0)))
        elif a[1] == 0:
            specs.append(pl.BlockSpec((rows, a[0].shape[1]), lambda j: (j, 0)))
        else:
            specs.append(pl.BlockSpec((a[0].shape[0], rows), lambda j: (0, j)))
    arrays = [a[0] if isinstance(a, tuple) else a for a in args]
    return pl.pallas_call(
        kernel,
        grid=(out[0] // rows,),
        in_specs=specs,
        out_specs=pl.BlockSpec((rows, out[1]), lambda j: (j, 0)),
        out_shape=jax.ShapeDtypeStruct(out, BF),
        scratch_shapes=scratch,
        input_output_aliases=dict(alias),
        compiler_params=ROOM,
        cost_estimate=pl.CostEstimate(flops=flops, bytes_accessed=6 * 2**20, transcendentals=0),
    )(*arrays)


def lines(first):
    groups = []
    for row in range(16):
        for i in range(8):
            line = [i * 8 + j if row % 2 == first else j * 8 + i for j in range(8)]
            groups.append([row * 64 + c for c in line])
    return groups


def exchange(block, groups):
    copies = jnp.broadcast_to(block[None], (8,) + block.shape)
    return lax.all_to_all(copies, ("prow", "pcol"), 0, 0, axis_index_groups=groups)


def hand_on(home, size):
    return lax.ppermute(home, "prow", [(i, i + size // 2) for i in range(0, 16, size)])


def step_of_panel(slab, pivots, l_top, l_panel_t):
    local_rows, w = slab.shape
    n = pivots.shape[0]
    k = l_panel_t.shape[0]
    row = lax.axis_index("prow").astype(jnp.int32)
    r = row.reshape(1)

    def picks(base):
        return pick(jnp.stack([row, base]), pivots, slab)

    near = exchange(l_panel_t, lines(0)).reshape(8 * k, local_rows)
    home = slab[:n]
    got = hand_on(home, 16)
    parts = inverse(l_top)
    got, parts = lax.optimization_barrier((got, parts))
    home = jnp.where(row == 0, home, got)
    got = hand_on(home, 8)
    picked, place, dest, most = picks(jnp.int32(0))
    near, picked = lax.optimization_barrier((near, picked))
    panel = exchange(near, lines(1)).reshape(n, local_rows)
    got, picked = lax.optimization_barrier((got, picked))
    home = jnp.where(row % 8 == 0, home, got)
    got = hand_on(home, 4)
    rows = lax.all_gather(picked, "prow", axis=0, tiled=True)
    got, rows = lax.optimization_barrier((got, rows))
    home = jnp.where(row % 4 == 0, home, got)
    sent = hand_on(home, 2)
    u, v = solve(place_solve_kernel, r, parts, place, rows)

    def in_rounds(_):
        def step(state):
            base, top = state
            picked, place, _, _ = picks(base)
            rows = lax.all_gather(picked, "prow", axis=0, tiled=True)
            top = pl.pallas_call(add_kernel, out_shape=jax.ShapeDtypeStruct((n, w), BF))(top, place, rows)
            return base + CAP, top

        _, top = lax.while_loop(lambda s: s[0] < most[0], step, (jnp.int32(0), jnp.zeros((n, w), BF)))
        return False, *solve(solve_kernel, r, parts, top)

    _, u, v = lax.while_loop(lambda s: s[0], in_rounds, (most[0] > CAP, u, v))
    flops = 2 * local_rows * n * w
    scratch = [pltpu.VMEM((n, w + 128), BF)]
    swapped = by_rows(swap_kernel, 256, slab.shape, (r, dest, home, sent, (slab, 0)), flops, scratch)
    return by_rows(update_kernel, 256, slab.shape, (r, (panel, 1), u, v, (swapped, 0)), flops, alias=[(4, 0)])


def solution(mesh):
    return jax.shard_map(
        step_of_panel,
        mesh=mesh,
        in_specs=(P("prow", "pcol"), P(), P(), P("pcol", "prow")),
        out_specs=P("prow", "pcol"),
        check_vma=False,
    )
```

```python
import jax
import jax.numpy as jnp
from jax import lax
from jax.experimental import pallas as pl
from jax.experimental.pallas import tpu as pltpu
from jax.sharding import PartitionSpec as P


BF, F32 = jnp.bfloat16, jnp.float32
HI = lax.Precision.HIGHEST


CAP = 80
ROOM = pltpu.CompilerParams(vmem_limit_bytes=20 * 2**20)


def column(row):
    n = row.shape[1]
    eye = lax.broadcasted_iota(jnp.int32, (n, n), 0) == lax.broadcasted_iota(jnp.int32, (n, n), 1)
    return jnp.sum(jnp.where(eye, row, 0.0), axis=1, keepdims=True)


def pick_kernel(where_ref, pivot_ref, slab_ref, pick_ref, place_ref, dest_ref, most_ref):
    n, rows = pivot_ref.shape[1], slab_ref.shape[0]
    me, base = where_ref[0], where_ref[1].astype(F32)
    p_int = pivot_ref[...]
    p_row = p_int.astype(F32)
    p_col = column(p_row)
    o_row = (p_int // rows).astype(F32)
    o_col = column(o_row)
    sub = lax.broadcasted_iota(jnp.int32, (n, n), 0)
    lane = lax.broadcasted_iota(jnp.int32, (n, n), 1)
    same = o_col == o_row
    rank_row = jnp.sum(jnp.where(same & (sub < lane), 1.0, 0.0), axis=0, keepdims=True)
    rank_col = jnp.sum(jnp.where(same & (lane < sub), 1.0, 0.0), axis=1, keepdims=True)
    most_ref[0] = jnp.max(rank_row).astype(jnp.int32) + 1
    slot = rank_col - base
    place_ref[...] = jnp.where((slot >= 0) & (slot < CAP), o_col * CAP + slot, -1.0).astype(jnp.int32)

    index = lax.broadcasted_iota(jnp.int32, (CAP, n), 0).astype(F32) + base
    chosen = (o_row == me.astype(F32)) & (rank_row == index)
    local = jnp.sum(jnp.where(chosen, p_row - (me * rows).astype(F32), 0.0), axis=1, keepdims=True)
    hot = lax.broadcasted_iota(jnp.int32, (CAP, rows), 1) == local.astype(jnp.int32)
    pick_ref[...] = jnp.dot(hot.astype(BF), slab_ref[...], preferred_element_type=F32).astype(BF)

    taken = jnp.where(p_col == lane.astype(F32), 1.0, 0.0)
    free_row = 1.0 - jnp.max(taken, axis=0, keepdims=True)
    free_col = column(free_row)
    far_row = jnp.where(p_row >= n, 1.0, 0.0)
    far_col = jnp.where(p_col >= n, 1.0, 0.0)
    free_rank = jnp.sum(jnp.where(sub < lane, free_col, 0.0), axis=0, keepdims=True)
    far_rank = jnp.sum(jnp.where(lane < sub, far_row, 0.0), axis=1, keepdims=True)
    match = (far_rank == free_rank) & (far_col > 0) & (free_row > 0)
    dest_ref[...] = (jnp.sum(jnp.where(match, p_col + 1.0, 0.0), axis=0, keepdims=True) - 1.0).astype(jnp.int32)


def pick(where, pivots, slab):
    n, w = pivots.shape[0], slab.shape[1]
    vmem = pl.BlockSpec(memory_space=pltpu.VMEM)
    return pl.pallas_call(
        pick_kernel,
        in_specs=[pl.BlockSpec(memory_space=pltpu.SMEM), vmem, vmem],
        out_shape=[
            jax.ShapeDtypeStruct((CAP, w), BF),
            jax.ShapeDtypeStruct((n, 1), jnp.int32),
            jax.ShapeDtypeStruct((1, n), jnp.int32),
            jax.ShapeDtypeStruct((1,), jnp.int32),
        ],
        out_specs=[vmem, vmem, vmem, pl.BlockSpec(memory_space=pltpu.SMEM)],
        compiler_params=ROOM,
        cost_estimate=pl.CostEstimate(flops=2 * 10**9, bytes_accessed=2 * slab.size, transcendentals=0),
    )(where, pivots[None], slab)


def mm(a, b):
    return jnp.dot(a, b, precision=HI, preferred_element_type=F32)


def inverse_kernel(l_ref, a_ref, b_ref, x_ref):
    n, t = l_ref.shape[0], 128
    row = lax.broadcasted_iota(jnp.int32, (t, t), 0)
    col = lax.broadcasted_iota(jnp.int32, (t, t), 1)
    eye = (row == col).astype(F32)
    x_ref[...] = jnp.zeros_like(x_ref)
    blocks = range(n // t)
    low = [
        jnp.where(row > col, l_ref[b * t : (b + 1) * t, b * t : (b + 1) * t].astype(F32), 0.0)
        for b in blocks
    ]
    step = 16
    near = [jnp.where(row // step == col // step, v, 0.0) for v in low]
    inv = [eye - v for v in near]
    power = near
    for _ in range(3):
        power = [mm(v, v) for v in power]
        inv = [x + mm(x, v) for x, v in zip(inv, power)]
    while step < t:
        off = [
            jnp.where((row // (2 * step) == col // (2 * step)) & (row // step != col // step), v, 0.0)
            for v in low
        ]
        half = [mm(x, v) for x, v in zip(inv, off)]
        inv = [x - mm(h, x) for x, h in zip(inv, half)]
        step *= 2
    for b in blocks:
        x_ref[b * t : (b + 1) * t, b * t : (b + 1) * t] = inv[b]
    size = t
    while size < n:
        for s in range(0, n, 2 * size):
            top, bot = slice(s, s + size), slice(s + size, s + 2 * size)
            x_ref[bot, top] = -mm(x_ref[bot, bot], mm(l_ref[bot, top].astype(F32), x_ref[top, top]))
        size *= 2
    x = x_ref[...]
    a = x.astype(BF)
    a_ref[...] = a
    b_ref[...] = (x - a.astype(F32)).astype(BF)


def inverse(l_top):
    n = l_top.shape[0]
    shape = jax.ShapeDtypeStruct((n, n), BF)
    return pl.pallas_call(
        inverse_kernel,
        out_shape=[shape] * 2,
        scratch_shapes=[pltpu.VMEM((n, n), F32)],
        compiler_params=ROOM,
        cost_estimate=pl.CostEstimate(flops=2 * 10**9, bytes_accessed=4 * n * n * 2, transcendentals=0),
    )(l_top)


def placed(place_ref, got_ref):
    hot = lax.broadcasted_iota(jnp.int32, (place_ref.shape[0], got_ref.shape[0]), 1) == place_ref[...]
    return jnp.dot(hot.astype(BF), got_ref[...], preferred_element_type=F32)


def finish(row_ref, a_ref, b_ref, top, u_ref, v_ref):
    u = jnp.dot(b_ref[...], top, preferred_element_type=F32)
    u += jnp.dot(a_ref[...], top, preferred_element_type=F32)
    u_ref[...] = u.astype(BF)
    for core in range(2):
        @pl.when(row_ref[0] % 2 == core)
        def _():
            order = [column_of(core, *b, *p) * 8 for p in NEXT for b in FAR]
            v_ref[...] = (-jnp.concatenate([u[i : i + 8] for i in order], axis=0)).astype(BF)


def place_solve_kernel(row_ref, a_ref, b_ref, place_ref, got_ref, u_ref, v_ref):
    finish(row_ref, a_ref, b_ref, placed(place_ref, got_ref).astype(BF), u_ref, v_ref)


def solve_kernel(row_ref, a_ref, b_ref, top_ref, u_ref, v_ref):
    finish(row_ref, a_ref, b_ref, top_ref[...], u_ref, v_ref)


def add_kernel(top_ref, place_ref, got_ref, out_ref):
    out_ref[...] = (top_ref[...].astype(F32) + placed(place_ref, got_ref)).astype(BF)


def solve(kernel, row, parts, *rest):
    n, w = parts[0].shape[0], rest[-1].shape[1]
    shape = jax.ShapeDtypeStruct((n, w), BF)
    vmem = pl.BlockSpec(memory_space=pltpu.VMEM)
    return tuple(pl.pallas_call(
        kernel,
        in_specs=[pl.BlockSpec(memory_space=pltpu.SMEM)] + [vmem] * (2 + len(rest)),
        out_shape=[shape] * 2,
        compiler_params=ROOM,
        cost_estimate=pl.CostEstimate(flops=10**9, bytes_accessed=10**7, transcendentals=0),
    )(row, *parts, *rest))


def update_kernel(row_ref, l_ref, u_ref, v_ref, dest_ref, own_ref, sent_ref, slab_ref, out_ref, right_ref):
    j = pl.program_id(0)
    rows, w = slab_ref.shape
    n = u_ref.shape[0]

    @pl.when(j == 0)
    def _():
        right_ref[:n, :w] = v_ref[...]
        right_ref[:n, w:] = jnp.zeros_like(right_ref[:n, w:])
        right_ref[n:, w:] = jnp.ones_like(right_ref[n:, w:])

        @pl.when(row_ref[0] % 2 == 0)
        def _():
            right_ref[n:, :w] = own_ref[...]

        @pl.when(row_ref[0] % 2 == 1)
        def _():
            right_ref[n:, :w] = sent_ref[...]

    first = (row_ref[0] * pl.num_programs(0) + j) * rows
    hit = first + lax.broadcasted_iota(jnp.int32, (rows, n), 0) == dest_ref[...]
    left = jnp.concatenate([l_ref[...].T, hit.astype(BF)], axis=1)
    acc = jnp.dot(left, right_ref[...], preferred_element_type=F32)
    lost = jnp.concatenate([acc[:, w:]] * (w // 128), axis=1)
    out_ref[...] = (jnp.where(lost > 0, 0.0, slab_ref[...].astype(F32)) + acc[:, :w]).astype(BF)

    @pl.when((row_ref[0] == 0) & (j == 0))
    def _():
        out_ref[:n, :] = u_ref[...]


def by_rows(kernel, rows, out, args, flops, scratch):
    specs = [pl.BlockSpec(memory_space=pltpu.SMEM)]
    for a in args[1:]:
        if not isinstance(a, tuple):
            specs.append(pl.BlockSpec(a.shape, lambda j: (0, 0)))
        elif a[1] == 0:
            specs.append(pl.BlockSpec((rows, a[0].shape[1]), lambda j: (j, 0)))
        else:
            specs.append(pl.BlockSpec((a[0].shape[0], rows), lambda j: (0, j)))
    arrays = [a[0] if isinstance(a, tuple) else a for a in args]
    return pl.pallas_call(
        kernel,
        grid=(out[0] // rows,),
        in_specs=specs,
        out_specs=pl.BlockSpec((rows, out[1]), lambda j: (j, 0)),
        out_shape=jax.ShapeDtypeStruct(out, BF),
        scratch_shapes=scratch,
        compiler_params=ROOM,
        cost_estimate=pl.CostEstimate(flops=flops, bytes_accessed=6 * 2**20, transcendentals=0),
    )(*arrays)


def chip(row, block, place):
    return (2 * block + place + row % 2) % 8


def column_of(row, bx, bz, px, pz):
    return chip(row, bx, px) * 8 + chip(row, bz, pz)


FAR = [(bx, bz) for bx in range(4) for bz in range(4)]
NEXT = [(px, pz) for px in range(2) for pz in range(2)]


def far_groups():
    return [[row * 64 + column_of(row, *b, *p) for b in FAR] for row in range(16) for p in NEXT]


def next_groups():
    return [[row * 64 + column_of(row, *b, *p) for p in NEXT] for row in range(16) for b in FAR]


def exchange(block, groups):
    copies = jnp.broadcast_to(block[None], (len(groups[0]),) + block.shape)
    return lax.all_to_all(copies, ("prow", "pcol"), 0, 0, axis_index_groups=groups)


def hand_on(home, size):
    return lax.ppermute(home, "prow", [(i, i + size // 2) for i in range(0, 16, size)])


def step_of_panel(slab, pivots, l_top, l_panel_t):
    local_rows, w = slab.shape
    n = pivots.shape[0]
    k = l_panel_t.shape[0]
    row = lax.axis_index("prow").astype(jnp.int32)
    r = row.reshape(1)

    def picks(base):
        return pick(jnp.stack([row, base]), pivots, slab)

    near = exchange(l_panel_t, far_groups()).reshape(16 * k, local_rows)
    home = slab[:n]
    got = hand_on(home, 16)
    got, l_top = lax.optimization_barrier((got, l_top))
    home = jnp.where(row == 0, home, got)
    got = hand_on(home, 8)
    parts = inverse(l_top)
    picked, place, dest, most = picks(jnp.int32(0))
    near, got, picked, parts = lax.optimization_barrier((near, got, picked, parts))
    home = jnp.where(row % 8 == 0, home, got)
    got = hand_on(home, 4)
    panel = exchange(near, next_groups()).reshape(n, local_rows)
    rows = lax.all_gather(picked, "prow", axis=0, tiled=True)
    got, rows = lax.optimization_barrier((got, rows))
    home = jnp.where(row % 4 == 0, home, got)
    sent = hand_on(home, 2)
    u, v = solve(place_solve_kernel, r, parts, place, rows)

    def in_rounds(_):
        def step(state):
            base, top = state
            picked, place, _, _ = picks(base)
            rows = lax.all_gather(picked, "prow", axis=0, tiled=True)
            top = pl.pallas_call(add_kernel, out_shape=jax.ShapeDtypeStruct((n, w), BF))(top, place, rows)
            return base + CAP, top

        _, top = lax.while_loop(lambda s: s[0] < most[0], step, (jnp.int32(0), jnp.zeros((n, w), BF)))
        return False, *solve(solve_kernel, r, parts, top)

    _, u, v = lax.while_loop(lambda s: s[0], in_rounds, (most[0] > CAP, u, v))
    flops = 4 * local_rows * n * w
    args = (r, (panel, 1), u, v, dest, home, sent, (slab, 0))
    return by_rows(update_kernel, 512, slab.shape, args, flops, [pltpu.VMEM((2 * n, w + 128), BF)])


def solution(mesh):
    return jax.shard_map(
        step_of_panel,
        mesh=mesh,
        in_specs=(P("prow", "pcol"), P(), P(), P("pcol", "prow")),
        out_specs=P("prow", "pcol"),
        check_vma=False,
    )
```

```python
import jax
import jax.numpy as jnp
from jax import lax
from jax.experimental import pallas as pl
from jax.experimental.pallas import tpu as pltpu
from jax.sharding import PartitionSpec as P


BF, F32 = jnp.bfloat16, jnp.float32
HI = lax.Precision.HIGHEST


CAP = 80
ROOM = pltpu.CompilerParams(vmem_limit_bytes=20 * 2**20)


def column(row):
    n = row.shape[1]
    eye = lax.broadcasted_iota(jnp.int32, (n, n), 0) == lax.broadcasted_iota(jnp.int32, (n, n), 1)
    return jnp.sum(jnp.where(eye, row, 0.0), axis=1, keepdims=True)


def pick_kernel(where_ref, pivot_ref, slab_ref, pick_ref, place_ref, dest_ref, most_ref):
    n, rows = pivot_ref.shape[1], slab_ref.shape[0]
    me, base = where_ref[0], where_ref[1].astype(F32)
    p_int = pivot_ref[...]
    p_row = p_int.astype(F32)
    p_col = column(p_row)
    o_row = (p_int // rows).astype(F32)
    o_col = column(o_row)
    sub = lax.broadcasted_iota(jnp.int32, (n, n), 0)
    lane = lax.broadcasted_iota(jnp.int32, (n, n), 1)
    same = o_col == o_row
    rank_row = jnp.sum(jnp.where(same & (sub < lane), 1.0, 0.0), axis=0, keepdims=True)
    rank_col = jnp.sum(jnp.where(same & (lane < sub), 1.0, 0.0), axis=1, keepdims=True)
    most_ref[0] = jnp.max(rank_row).astype(jnp.int32) + 1
    slot = rank_col - base
    place_ref[...] = jnp.where((slot >= 0) & (slot < CAP), o_col * CAP + slot, -1.0).astype(jnp.int32)

    index = lax.broadcasted_iota(jnp.int32, (CAP, n), 0).astype(F32) + base
    chosen = (o_row == me.astype(F32)) & (rank_row == index)
    local = jnp.sum(jnp.where(chosen, p_row - (me * rows).astype(F32), 0.0), axis=1, keepdims=True)
    hot = lax.broadcasted_iota(jnp.int32, (CAP, rows), 1) == local.astype(jnp.int32)
    pick_ref[...] = jnp.dot(hot.astype(BF), slab_ref[...], preferred_element_type=F32).astype(BF)

    taken = jnp.where(p_col == lane.astype(F32), 1.0, 0.0)
    free_row = 1.0 - jnp.max(taken, axis=0, keepdims=True)
    free_col = column(free_row)
    far_row = jnp.where(p_row >= n, 1.0, 0.0)
    far_col = jnp.where(p_col >= n, 1.0, 0.0)
    free_rank = jnp.sum(jnp.where(sub < lane, free_col, 0.0), axis=0, keepdims=True)
    far_rank = jnp.sum(jnp.where(lane < sub, far_row, 0.0), axis=1, keepdims=True)
    match = (far_rank == free_rank) & (far_col > 0) & (free_row > 0)
    dest_ref[...] = (jnp.sum(jnp.where(match, p_col + 1.0, 0.0), axis=0, keepdims=True) - 1.0).astype(jnp.int32)


def pick(where, pivots, slab):
    n, w = pivots.shape[0], slab.shape[1]
    vmem = pl.BlockSpec(memory_space=pltpu.VMEM)
    return pl.pallas_call(
        pick_kernel,
        in_specs=[pl.BlockSpec(memory_space=pltpu.SMEM), vmem, vmem],
        out_shape=[
            jax.ShapeDtypeStruct((CAP, w), BF),
            jax.ShapeDtypeStruct((n, 1), jnp.int32),
            jax.ShapeDtypeStruct((1, n), jnp.int32),
            jax.ShapeDtypeStruct((1,), jnp.int32),
        ],
        out_specs=[vmem, vmem, vmem, pl.BlockSpec(memory_space=pltpu.SMEM)],
        compiler_params=ROOM,
        cost_estimate=pl.CostEstimate(flops=2 * 10**9, bytes_accessed=2 * slab.size, transcendentals=0),
    )(where, pivots[None], slab)


def mm(a, b):
    return jnp.dot(a, b, precision=HI, preferred_element_type=F32)


def inverse_kernel(l_ref, a_ref, b_ref, x_ref):
    n, t = l_ref.shape[0], 128
    row = lax.broadcasted_iota(jnp.int32, (t, t), 0)
    col = lax.broadcasted_iota(jnp.int32, (t, t), 1)
    eye = (row == col).astype(F32)
    x_ref[...] = jnp.zeros_like(x_ref)
    blocks = range(n // t)
    low = [
        jnp.where(row > col, l_ref[b * t : (b + 1) * t, b * t : (b + 1) * t].astype(F32), 0.0)
        for b in blocks
    ]
    step = 16
    near = [jnp.where(row // step == col // step, v, 0.0) for v in low]
    inv = [eye - v for v in near]
    power = near
    for _ in range(3):
        power = [mm(v, v) for v in power]
        inv = [x + mm(x, v) for x, v in zip(inv, power)]
    while step < t:
        off = [
            jnp.where((row // (2 * step) == col // (2 * step)) & (row // step != col // step), v, 0.0)
            for v in low
        ]
        half = [mm(x, v) for x, v in zip(inv, off)]
        inv = [x - mm(h, x) for x, h in zip(inv, half)]
        step *= 2
    for b in blocks:
        x_ref[b * t : (b + 1) * t, b * t : (b + 1) * t] = inv[b]
    size = t
    while size < n:
        for s in range(0, n, 2 * size):
            top, bot = slice(s, s + size), slice(s + size, s + 2 * size)
            x_ref[bot, top] = -mm(x_ref[bot, bot], mm(l_ref[bot, top].astype(F32), x_ref[top, top]))
        size *= 2
    x = x_ref[...]
    a = x.astype(BF)
    a_ref[...] = a
    b_ref[...] = (x - a.astype(F32)).astype(BF)


def inverse(l_top):
    n = l_top.shape[0]
    shape = jax.ShapeDtypeStruct((n, n), BF)
    return pl.pallas_call(
        inverse_kernel,
        out_shape=[shape] * 2,
        scratch_shapes=[pltpu.VMEM((n, n), F32)],
        compiler_params=ROOM,
        cost_estimate=pl.CostEstimate(flops=2 * 10**9, bytes_accessed=4 * n * n * 2, transcendentals=0),
    )(l_top)


def placed(place_ref, got_ref):
    hot = lax.broadcasted_iota(jnp.int32, (place_ref.shape[0], got_ref.shape[0]), 1) == place_ref[...]
    return jnp.dot(hot.astype(BF), got_ref[...], preferred_element_type=F32)


def finish(row_ref, a_ref, b_ref, top, u_ref, v_ref):
    u = jnp.dot(b_ref[...], top, preferred_element_type=F32)
    u += jnp.dot(a_ref[...], top, preferred_element_type=F32)
    u_ref[...] = u.astype(BF)
    for core in range(2):
        @pl.when(row_ref[0] % 2 == core)
        def _():
            order = [column_of(core, *b, *p) * 8 for p in NEXT for b in FAR]
            v_ref[...] = (-jnp.concatenate([u[i : i + 8] for i in order], axis=0)).astype(BF)


def place_solve_kernel(row_ref, a_ref, b_ref, place_ref, got_ref, u_ref, v_ref, top_ref):
    top = placed(place_ref, got_ref).astype(BF)
    top_ref[...] = top
    finish(row_ref, a_ref, b_ref, top, u_ref, v_ref)


def solve_kernel(row_ref, a_ref, b_ref, top_ref, u_ref, v_ref):
    finish(row_ref, a_ref, b_ref, top_ref[...], u_ref, v_ref)


def add_kernel(top_ref, place_ref, got_ref, out_ref):
    out_ref[...] = (top_ref[...].astype(F32) + placed(place_ref, got_ref)).astype(BF)


def solve(kernel, row, parts, *rest):
    n, w = parts[0].shape[0], rest[-1].shape[1]
    shape = jax.ShapeDtypeStruct((n, w), BF)
    vmem = pl.BlockSpec(memory_space=pltpu.VMEM)
    return tuple(pl.pallas_call(
        kernel,
        in_specs=[pl.BlockSpec(memory_space=pltpu.SMEM)] + [vmem] * (2 + len(rest)),
        out_shape=[shape] * (3 if kernel is place_solve_kernel else 2),
        compiler_params=ROOM,
        cost_estimate=pl.CostEstimate(flops=10**9, bytes_accessed=10**7, transcendentals=0),
    )(row, *parts, *rest))


def update_kernel(row_ref, l_ref, u_ref, v_ref, dest_ref, own_ref, sent_ref, slab_ref, out_ref, right_ref):
    j = pl.program_id(0)
    rows, w = slab_ref.shape
    n = u_ref.shape[0]

    @pl.when(j == 0)
    def _():
        right_ref[:n, :w] = v_ref[...]
        right_ref[:n, w:] = jnp.zeros_like(right_ref[:n, w:])
        right_ref[n:, w:] = jnp.ones_like(right_ref[n:, w:])

        @pl.when(row_ref[0] % 2 == 0)
        def _():
            right_ref[n:, :w] = own_ref[...]

        @pl.when(row_ref[0] % 2 == 1)
        def _():
            right_ref[n:, :w] = sent_ref[...]

    first = (row_ref[0] * pl.num_programs(0) + j) * rows
    hit = first + lax.broadcasted_iota(jnp.int32, (rows, n), 0) == dest_ref[...]
    left = jnp.concatenate([l_ref[...].T, hit.astype(BF)], axis=1)
    acc = jnp.dot(left, right_ref[...], preferred_element_type=F32)
    lost = jnp.concatenate([acc[:, w:]] * (w // 128), axis=1)
    out_ref[...] = (jnp.where(lost > 0, 0.0, slab_ref[...].astype(F32)) + acc[:, :w]).astype(BF)

    @pl.when((row_ref[0] == 0) & (j == 0))
    def _():
        out_ref[:n, :] = u_ref[...]


def by_rows(kernel, rows, out, args, flops, scratch):
    specs = [pl.BlockSpec(memory_space=pltpu.SMEM)]
    for a in args[1:]:
        if not isinstance(a, tuple):
            specs.append(pl.BlockSpec(a.shape, lambda j: (0, 0)))
        elif a[1] == 0:
            specs.append(pl.BlockSpec((rows, a[0].shape[1]), lambda j: (j, 0)))
        else:
            specs.append(pl.BlockSpec((a[0].shape[0], rows), lambda j: (0, j)))
    arrays = [a[0] if isinstance(a, tuple) else a for a in args]
    return pl.pallas_call(
        kernel,
        grid=(out[0] // rows,),
        in_specs=specs,
        out_specs=pl.BlockSpec((rows, out[1]), lambda j: (j, 0)),
        out_shape=jax.ShapeDtypeStruct(out, BF),
        scratch_shapes=scratch,
        compiler_params=ROOM,
        cost_estimate=pl.CostEstimate(flops=flops, bytes_accessed=6 * 2**20, transcendentals=0),
    )(*arrays)


def chip(row, block, place):
    return (2 * block + place + row % 2) % 8


def column_of(row, bx, bz, px, pz):
    return chip(row, bx, px) * 8 + chip(row, bz, pz)


FAR = [(bx, bz) for bx in range(4) for bz in range(4)]
NEXT = [(px, pz) for px in range(2) for pz in range(2)]


def far_groups():
    return [[row * 64 + column_of(row, *b, *p) for b in FAR] for row in range(16) for p in NEXT]


def next_groups():
    return [[row * 64 + column_of(row, *b, *p) for p in NEXT] for row in range(16) for b in FAR]


def exchange(block, groups):
    copies = jnp.broadcast_to(block[None], (len(groups[0]),) + block.shape)
    return lax.all_to_all(copies, ("prow", "pcol"), 0, 0, axis_index_groups=groups)


def hand_on(home, size):
    return lax.ppermute(home, "prow", [(i, i + size // 2) for i in range(0, 16, size)])


def step_of_panel(slab, pivots, l_top, l_panel_t):
    local_rows, w = slab.shape
    n = pivots.shape[0]
    k = l_panel_t.shape[0]
    row = lax.axis_index("prow").astype(jnp.int32)
    r = row.reshape(1)

    def picks(base):
        return pick(jnp.stack([row, base]), pivots, slab)

    near = exchange(l_panel_t, far_groups()).reshape(16 * k, local_rows)
    home = slab[:n]
    got = hand_on(home, 16)
    picked, place, dest, most = picks(jnp.int32(0))
    rows = lax.all_gather(picked, "prow", axis=0, tiled=True)
    near, got, rows, l_top = lax.optimization_barrier((near, got, rows, l_top))
    panel = exchange(near, next_groups()).reshape(n, local_rows)
    home = jnp.where(row == 0, home, got)
    got = hand_on(home, 8)
    parts = inverse(l_top)
    got, parts = lax.optimization_barrier((got, parts))
    home = jnp.where(row % 8 == 0, home, got)
    got = hand_on(home, 4)
    u, v, top = solve(place_solve_kernel, r, parts, place, rows)
    got, u = lax.optimization_barrier((got, u))
    home = jnp.where(row % 4 == 0, home, got)
    sent = hand_on(home, 2)

    def further(state):
        base, top, _, _ = state
        picked, place, _, _ = picks(base)
        rows = lax.all_gather(picked, "prow", axis=0, tiled=True)
        top = pl.pallas_call(add_kernel, out_shape=jax.ShapeDtypeStruct((n, w), BF))(top, place, rows)
        return base + CAP, top, *solve(solve_kernel, r, parts, top)

    _, _, u, v = lax.while_loop(lambda s: s[0] < most[0], further, (jnp.int32(CAP), top, u, v))
    flops = 4 * local_rows * n * w
    args = (r, (panel, 1), u, v, dest, home, sent, (slab, 0))
    return by_rows(update_kernel, 512, slab.shape, args, flops, [pltpu.VMEM((2 * n, w + 128), BF)])


def solution(mesh):
    return jax.shard_map(
        step_of_panel,
        mesh=mesh,
        in_specs=(P("prow", "pcol"), P(), P(), P("pcol", "prow")),
        out_specs=P("prow", "pcol"),
        check_vma=False,
    )
```

```python
import jax
import jax.numpy as jnp
from jax import lax
from jax.experimental import pallas as pl
from jax.experimental.pallas import tpu as pltpu
from jax.sharding import PartitionSpec as P


BF, F32 = jnp.bfloat16, jnp.float32
HI = lax.Precision.HIGHEST


CAP = 80
ROOM = pltpu.CompilerParams(vmem_limit_bytes=20 * 2**20)


def column(row):
    n = row.shape[1]
    eye = lax.broadcasted_iota(jnp.int32, (n, n), 0) == lax.broadcasted_iota(jnp.int32, (n, n), 1)
    return jnp.sum(jnp.where(eye, row, 0.0), axis=1, keepdims=True)


def pick_kernel(where_ref, pivot_ref, slab_ref, pick_ref, place_ref, dest_ref, most_ref):
    n, rows = pivot_ref.shape[1], slab_ref.shape[0]
    me, base = where_ref[0], where_ref[1].astype(F32)
    p_int = pivot_ref[...]
    p_row = p_int.astype(F32)
    p_col = column(p_row)
    o_row = (p_int // rows).astype(F32)
    o_col = column(o_row)
    sub = lax.broadcasted_iota(jnp.int32, (n, n), 0)
    lane = lax.broadcasted_iota(jnp.int32, (n, n), 1)
    same = o_col == o_row
    rank_row = jnp.sum(jnp.where(same & (sub < lane), 1.0, 0.0), axis=0, keepdims=True)
    rank_col = jnp.sum(jnp.where(same & (lane < sub), 1.0, 0.0), axis=1, keepdims=True)
    most_ref[0] = jnp.max(rank_row).astype(jnp.int32) + 1
    slot = rank_col - base
    place_ref[...] = jnp.where((slot >= 0) & (slot < CAP), o_col * CAP + slot, -1.0).astype(jnp.int32)

    index = lax.broadcasted_iota(jnp.int32, (CAP, n), 0).astype(F32) + base
    chosen = (o_row == me.astype(F32)) & (rank_row == index)
    local = jnp.sum(jnp.where(chosen, p_row - (me * rows).astype(F32), 0.0), axis=1, keepdims=True)
    hot = lax.broadcasted_iota(jnp.int32, (CAP, rows), 1) == local.astype(jnp.int32)
    pick_ref[...] = jnp.dot(hot.astype(BF), slab_ref[...], preferred_element_type=F32).astype(BF)

    taken = jnp.where(p_col == lane.astype(F32), 1.0, 0.0)
    free_row = 1.0 - jnp.max(taken, axis=0, keepdims=True)
    free_col = column(free_row)
    far_row = jnp.where(p_row >= n, 1.0, 0.0)
    far_col = jnp.where(p_col >= n, 1.0, 0.0)
    free_rank = jnp.sum(jnp.where(sub < lane, free_col, 0.0), axis=0, keepdims=True)
    far_rank = jnp.sum(jnp.where(lane < sub, far_row, 0.0), axis=1, keepdims=True)
    match = (far_rank == free_rank) & (far_col > 0) & (free_row > 0)
    dest_ref[...] = (jnp.sum(jnp.where(match, p_col + 1.0, 0.0), axis=0, keepdims=True) - 1.0).astype(jnp.int32)


def pick(where, pivots, slab):
    n, w = pivots.shape[0], slab.shape[1]
    vmem = pl.BlockSpec(memory_space=pltpu.VMEM)
    return pl.pallas_call(
        pick_kernel,
        in_specs=[pl.BlockSpec(memory_space=pltpu.SMEM), vmem, vmem],
        out_shape=[
            jax.ShapeDtypeStruct((CAP, w), BF),
            jax.ShapeDtypeStruct((n, 1), jnp.int32),
            jax.ShapeDtypeStruct((1, n), jnp.int32),
            jax.ShapeDtypeStruct((1,), jnp.int32),
        ],
        out_specs=[vmem, vmem, vmem, pl.BlockSpec(memory_space=pltpu.SMEM)],
        compiler_params=ROOM,
        cost_estimate=pl.CostEstimate(flops=2 * 10**9, bytes_accessed=2 * slab.size, transcendentals=0),
    )(where, pivots[None], slab)


def mm(a, b):
    return jnp.dot(a, b, precision=HI, preferred_element_type=F32)


def inverse_kernel(l_ref, a_ref, b_ref, x_ref):
    n, t = l_ref.shape[0], 128
    row = lax.broadcasted_iota(jnp.int32, (t, t), 0)
    col = lax.broadcasted_iota(jnp.int32, (t, t), 1)
    eye = (row == col).astype(F32)
    x_ref[...] = jnp.zeros_like(x_ref)
    blocks = range(n // t)
    low = [
        jnp.where(row > col, l_ref[b * t : (b + 1) * t, b * t : (b + 1) * t].astype(F32), 0.0)
        for b in blocks
    ]
    step = 16
    near = [jnp.where(row // step == col // step, v, 0.0) for v in low]
    inv = [eye - v for v in near]
    power = near
    for _ in range(3):
        power = [mm(v, v) for v in power]
        inv = [x + mm(x, v) for x, v in zip(inv, power)]
    while step < t:
        off = [
            jnp.where((row // (2 * step) == col // (2 * step)) & (row // step != col // step), v, 0.0)
            for v in low
        ]
        half = [mm(x, v) for x, v in zip(inv, off)]
        inv = [x - mm(h, x) for x, h in zip(inv, half)]
        step *= 2
    for b in blocks:
        x_ref[b * t : (b + 1) * t, b * t : (b + 1) * t] = inv[b]
    size = t
    while size < n:
        for s in range(0, n, 2 * size):
            top, bot = slice(s, s + size), slice(s + size, s + 2 * size)
            x_ref[bot, top] = -mm(x_ref[bot, bot], mm(l_ref[bot, top].astype(F32), x_ref[top, top]))
        size *= 2
    x = x_ref[...]
    a = x.astype(BF)
    a_ref[...] = a
    b_ref[...] = (x - a.astype(F32)).astype(BF)


def inverse(l_top):
    n = l_top.shape[0]
    shape = jax.ShapeDtypeStruct((n, n), BF)
    return pl.pallas_call(
        inverse_kernel,
        out_shape=[shape] * 2,
        scratch_shapes=[pltpu.VMEM((n, n), F32)],
        compiler_params=ROOM,
        cost_estimate=pl.CostEstimate(flops=2 * 10**9, bytes_accessed=4 * n * n * 2, transcendentals=0),
    )(l_top)


def placed(place_ref, got_ref):
    hot = lax.broadcasted_iota(jnp.int32, (place_ref.shape[0], got_ref.shape[0]), 1) == place_ref[...]
    return jnp.dot(hot.astype(BF), got_ref[...], preferred_element_type=F32)


def finish(row_ref, a_ref, b_ref, top, u_ref, v_ref):
    u = jnp.dot(b_ref[...], top, preferred_element_type=F32)
    u += jnp.dot(a_ref[...], top, preferred_element_type=F32)
    u_ref[...] = u.astype(BF)
    for core in range(2):
        @pl.when(row_ref[0] % 2 == core)
        def _():
            order = [column_of(core, *b, *p) * 8 for p in NEXT for b in FAR]
            v_ref[...] = (-jnp.concatenate([u[i : i + 8] for i in order], axis=0)).astype(BF)


def place_solve_kernel(row_ref, a_ref, b_ref, place_ref, got_ref, u_ref, v_ref, top_ref):
    top = placed(place_ref, got_ref).astype(BF)
    top_ref[...] = top
    finish(row_ref, a_ref, b_ref, top, u_ref, v_ref)


def solve_kernel(row_ref, a_ref, b_ref, top_ref, u_ref, v_ref):
    finish(row_ref, a_ref, b_ref, top_ref[...], u_ref, v_ref)


def add_kernel(top_ref, place_ref, got_ref, out_ref):
    out_ref[...] = (top_ref[...].astype(F32) + placed(place_ref, got_ref)).astype(BF)


def solve(kernel, row, parts, *rest):
    n, w = parts[0].shape[0], rest[-1].shape[1]
    shape = jax.ShapeDtypeStruct((n, w), BF)
    vmem = pl.BlockSpec(memory_space=pltpu.VMEM)
    return tuple(pl.pallas_call(
        kernel,
        in_specs=[pl.BlockSpec(memory_space=pltpu.SMEM)] + [vmem] * (2 + len(rest)),
        out_shape=[shape] * (3 if kernel is place_solve_kernel else 2),
        compiler_params=ROOM,
        cost_estimate=pl.CostEstimate(flops=10**9, bytes_accessed=10**7, transcendentals=0),
    )(row, *parts, *rest))


def update_kernel(row_ref, l_ref, u_ref, v_ref, dest_ref, own_ref, sent_ref, slab_ref, out_ref, right_ref):
    j = pl.program_id(0)
    rows, w = slab_ref.shape
    n = u_ref.shape[0]

    @pl.when(j == 0)
    def _():
        right_ref[:n, :w] = v_ref[...]
        right_ref[:n, w:] = jnp.zeros_like(right_ref[:n, w:])
        right_ref[n:, w:] = jnp.ones_like(right_ref[n:, w:])

        @pl.when(row_ref[0] % 2 == 0)
        def _():
            right_ref[n:, :w] = own_ref[...]

        @pl.when(row_ref[0] % 2 == 1)
        def _():
            right_ref[n:, :w] = sent_ref[...]

    first = (row_ref[0] * pl.num_programs(0) + j) * rows
    hit = first + lax.broadcasted_iota(jnp.int32, (rows, n), 0) == dest_ref[...]
    left = jnp.concatenate([l_ref[...].T, hit.astype(BF)], axis=1)
    acc = jnp.dot(left, right_ref[...], preferred_element_type=F32)
    lost = jnp.concatenate([acc[:, w:]] * (w // 128), axis=1)
    out_ref[...] = (jnp.where(lost > 0, 0.0, slab_ref[...].astype(F32)) + acc[:, :w]).astype(BF)

    @pl.when((row_ref[0] == 0) & (j == 0))
    def _():
        out_ref[:n, :] = u_ref[...]


def by_rows(kernel, rows, out, args, flops, scratch):
    specs = [pl.BlockSpec(memory_space=pltpu.SMEM)]
    for a in args[1:]:
        if not isinstance(a, tuple):
            specs.append(pl.BlockSpec(a.shape, lambda j: (0, 0)))
        elif a[1] == 0:
            specs.append(pl.BlockSpec((rows, a[0].shape[1]), lambda j: (j, 0)))
        else:
            specs.append(pl.BlockSpec((a[0].shape[0], rows), lambda j: (0, j)))
    arrays = [a[0] if isinstance(a, tuple) else a for a in args]
    return pl.pallas_call(
        kernel,
        grid=(out[0] // rows,),
        in_specs=specs,
        out_specs=pl.BlockSpec((rows, out[1]), lambda j: (j, 0)),
        out_shape=jax.ShapeDtypeStruct(out, BF),
        scratch_shapes=scratch,
        compiler_params=ROOM,
        cost_estimate=pl.CostEstimate(flops=flops, bytes_accessed=6 * 2**20, transcendentals=0),
    )(*arrays)


def chip(row, block, place):
    return (2 * block + place + row % 2) % 8


def column_of(row, bx, bz, px, pz):
    return chip(row, bx, px) * 8 + chip(row, bz, pz)


FAR = [(bx, bz) for bx in range(4) for bz in range(4)]
NEXT = [(px, pz) for px in range(2) for pz in range(2)]


def far_groups():
    return [[row * 64 + column_of(row, *b, *p) for b in FAR] for row in range(16) for p in NEXT]


def next_groups():
    return [[row * 64 + column_of(row, *b, *p) for p in NEXT] for row in range(16) for b in FAR]


def exchange(block, groups):
    copies = jnp.broadcast_to(block[None], (len(groups[0]),) + block.shape)
    return lax.all_to_all(copies, ("prow", "pcol"), 0, 0, axis_index_groups=groups)


def hand_on(home, size):
    return lax.ppermute(home, "prow", [(i, i + size // 2) for i in range(0, 16, size)])


def step_of_panel(slab, pivots, l_top, l_panel_t):
    local_rows, w = slab.shape
    n = pivots.shape[0]
    k = l_panel_t.shape[0]
    row = lax.axis_index("prow").astype(jnp.int32)
    r = row.reshape(1)

    def picks(base):
        return pick(jnp.stack([row, base]), pivots, slab)

    near = exchange(l_panel_t, far_groups()).reshape(16 * k, local_rows)
    home = slab[:n]
    got = hand_on(home, 16)
    got, l_top = lax.optimization_barrier((got, l_top))
    home = jnp.where(row == 0, home, got)
    got = hand_on(home, 8)
    parts = inverse(l_top)
    picked, place, dest, most = picks(jnp.int32(0))
    near, got, picked, parts = lax.optimization_barrier((near, got, picked, parts))
    home = jnp.where(row % 8 == 0, home, got)
    got = hand_on(home, 4)
    panel = exchange(near, next_groups()).reshape(n, local_rows)
    rows = lax.all_gather(picked, "prow", axis=0, tiled=True)
    got, rows = lax.optimization_barrier((got, rows))
    home = jnp.where(row % 4 == 0, home, got)
    sent = hand_on(home, 2)
    u, v, top = solve(place_solve_kernel, r, parts, place, rows)

    def further(state):
        base, top, _, _ = state
        picked, place, _, _ = picks(base)
        rows = lax.all_gather(picked, "prow", axis=0, tiled=True)
        top = pl.pallas_call(add_kernel, out_shape=jax.ShapeDtypeStruct((n, w), BF))(top, place, rows)
        return base + CAP, top, *solve(solve_kernel, r, parts, top)

    _, _, u, v = lax.while_loop(lambda s: s[0] < most[0], further, (jnp.int32(CAP), top, u, v))
    flops = 4 * local_rows * n * w
    args = (r, (panel, 1), u, v, dest, home, sent, (slab, 0))
    return by_rows(update_kernel, 512, slab.shape, args, flops, [pltpu.VMEM((2 * n, w + 128), BF)])


def solution(mesh):
    return jax.shard_map(
        step_of_panel,
        mesh=mesh,
        in_specs=(P("prow", "pcol"), P(), P(), P("pcol", "prow")),
        out_specs=P("prow", "pcol"),
        check_vma=False,
    )
```
